32 devices in a mesh: member: 1 (over z), lon: 4 (over y), lat: 8 (over x, core).
Axes of the slice: x: 4, y: 4, z: 1, core: 2. Of those that a mesh axis runs over, the one named last changes fastest.
The devices are a block of a 4x4x8 slice.
Arguments:
- field_in: float32 [4, 256, 256, 512], P('member', None, 'lat', 'lon')
- fwd_table: float32 [256, 256, 256], replicated
- inv_table: float32 [256, 256, 256], replicated
- mix_weights: float32 [256, 256, 256, 2], replicated
Outputs:
- output: float32 [4, 256, 256, 512], P('member', None, 'lat', 'lon')
All inputs are finite; a program needn't handle non-finite values.
Results may differ from the reference program's by a relative error of at most 0.00315129.
Values are sent between devices in bfloat16 or wider.
A program may use at most 768 MiB of HBM per device.

```python
import math
import jax
import jax.numpy as jnp
from jax import lax

SAMPLES = 4
CHANNELS = 256
LATITUDES = 256
DEGREES = 256
LONGITUDES = 2 * LATITUDES


def as_bf16(values):
    return values.astype(jnp.bfloat16).astype(jnp.float32)


def legendre_table(colatitude):
    cos_t = jnp.cos(colatitude)
    log_sin = jnp.log(jnp.sin(colatitude))
    orders = jnp.arange(DEGREES).astype(jnp.float32)
    log_steps = jnp.cumsum(jnp.log((2.0 * orders + 1.0) / (2.0 * orders + 2.0)))
    log_prod = jnp.concatenate([jnp.zeros((1,), jnp.float32), log_steps[:-1]])
    log_diag = 0.5 * (jnp.log((2.0 * orders + 1.0) / (4.0 * math.pi)) + log_prod)
    diag_vals = jnp.exp(log_diag[:, None] + orders[:, None] * log_sin[None, :])

    def degree_step(carry_vals, degree):
        prev_two, prev_one = carry_vals
        deg_f = degree.astype(jnp.float32)
        coef_a = jnp.sqrt(jnp.maximum(4.0 * deg_f * deg_f - 1.0, 0.0) / jnp.maximum(deg_f * deg_f - orders * orders, 1.0))
        prev_f = deg_f - 1.0
        coef_b = jnp.sqrt(jnp.maximum(prev_f * prev_f - orders * orders, 0.0) / jnp.maximum(4.0 * prev_f * prev_f - 1.0, 1.0))
        recur_val = coef_a[:, None] * (cos_t[None, :] * prev_one - coef_b[:, None] * prev_two)
        next_val = jnp.where((deg_f == orders)[:, None], diag_vals, jnp.where((deg_f > orders)[:, None], recur_val, 0.0))
        return (prev_one, next_val), next_val

    zero_rows = jnp.zeros((DEGREES, LATITUDES), jnp.float32)
    _, leg_table = lax.scan(degree_step, (zero_rows, zero_rows), jnp.arange(DEGREES))
    return jnp.transpose(leg_table, (1, 0, 2))


def setup_inputs(seed: int = 0, part: int = 0) -> dict:
    root_key = jax.random.key(seed)
    key_field, key_fwd, key_inv, key_mix = jax.random.split(root_key, 4)
    key_part = jax.random.fold_in(key_field, part)
    key_noise, key_smooth = jax.random.split(key_part, 2)
    colatitude = math.pi * (jnp.arange(LATITUDES).astype(jnp.float32) + 0.5) / LATITUDES
    longitude = (2.0 * math.pi / LONGITUDES) * jnp.arange(LONGITUDES).astype(jnp.float32)
    smooth_coef = jax.random.normal(key_smooth, (SAMPLES, CHANNELS, 3, 1, 1), jnp.float32)
    smooth = smooth_coef[:, :, 0] * jnp.cos(colatitude)[:, None] + jnp.sin(colatitude)[:, None] * (smooth_coef[:, :, 1] * jnp.cos(longitude) + smooth_coef[:, :, 2] * jnp.sin(longitude))
    white_noise = jax.random.normal(key_noise, (SAMPLES, CHANNELS, LATITUDES, LONGITUDES), jnp.float32)
    field_in = smooth + white_noise
    leg_table = legendre_table(colatitude)
    quad_weights = (2.0 * math.pi / LONGITUDES) * (math.pi / LATITUDES) * jnp.sin(colatitude)
    table_shape = (DEGREES, DEGREES, LATITUDES)
    fwd_table = leg_table * quad_weights * (1.0 + 0.3 * jax.random.uniform(key_fwd, table_shape, jnp.float32, -1.0, 1.0))
    inv_table = leg_table * (1.0 + 0.3 * jax.random.uniform(key_inv, table_shape, jnp.float32, -1.0, 1.0))
    mix_scale = LATITUDES / (DEGREES * math.sqrt(CHANNELS))
    mix_weights = mix_scale * jax.random.normal(key_mix, (DEGREES, CHANNELS, CHANNELS, 2), jnp.float32)
    return {'field_in': field_in, 'fwd_table': fwd_table, 'inv_table': inv_table, 'mix_weights': mix_weights}


def reference(field_in, fwd_table, inv_table, mix_weights):
    lon_ids = jnp.arange(LONGITUDES)
    wave_ids = jnp.arange(DEGREES)
    phase_arg = (2.0 * math.pi / LONGITUDES) * ((lon_ids[:, None] * wave_ids[None, :]) % LONGITUDES).astype(jnp.float32)
    weight_m = jnp.where(wave_ids == 0, 1.0, 2.0).astype(jnp.float32)
    cos_fwd = as_bf16(jnp.cos(phase_arg))
    sin_fwd = as_bf16(-jnp.sin(phase_arg))
    cos_inv = as_bf16(weight_m * jnp.cos(phase_arg))
    sin_inv = as_bf16(-weight_m * jnp.sin(phase_arg))
    fwd_bf = as_bf16(fwd_table)
    inv_bf = as_bf16(inv_table)
    w_re = as_bf16(mix_weights[..., 0])
    w_im = as_bf16(mix_weights[..., 1])

    def one_sample(sample):
        grid_val = as_bf16(sample)
        spec_re = as_bf16(jnp.einsum('ctj,jm->ctm', grid_val, cos_fwd))
        spec_im = as_bf16(jnp.einsum('ctj,jm->ctm', grid_val, sin_fwd))
        coef_re = as_bf16(jnp.einsum('mlt,ctm->clm', fwd_bf, spec_re))
        coef_im = as_bf16(jnp.einsum('mlt,ctm->clm', fwd_bf, spec_im))
        mixed_re = as_bf16(jnp.einsum('loi,ilm->olm', w_re, coef_re) - jnp.einsum('loi,ilm->olm', w_im, coef_im))
        mixed_im = as_bf16(jnp.einsum('loi,ilm->olm', w_re, coef_im) + jnp.einsum('loi,ilm->olm', w_im, coef_re))
        back_re = as_bf16(jnp.einsum('mlt,clm->ctm', inv_bf, mixed_re))
        back_im = as_bf16(jnp.einsum('mlt,clm->ctm', inv_bf, mixed_im))
        wave_grid = as_bf16(jnp.einsum('ctm,jm->ctj', back_re, cos_inv) + jnp.einsum('ctm,jm->ctj', back_im, sin_inv))
        return sample + jax.nn.gelu(wave_grid, approximate=True)

    return lax.map(one_sample, field_in)
```

```python
import functools
import math
import jax
import jax.numpy as jnp
from jax import lax
from jax.experimental import pallas as pl
from jax.experimental.pallas import tpu as pltpu
from jax.sharding import PartitionSpec as P

MESH = pl.DeviceIdType.MESH
ROWS = 16
LANES = 128
VMEM_LIMIT = 66000000


def row_waves(degrees, lat_count):
    m_loc = degrees // lat_count
    groups = m_loc // ROWS
    waves = jnp.arange(degrees).reshape(lat_count, groups, 1, ROWS)
    waves = jnp.broadcast_to(waves, (lat_count, groups, 2, ROWS)).reshape(-1)
    part = jnp.broadcast_to(jnp.arange(2).reshape(1, 1, 2, 1), (lat_count, groups, 2, ROWS)).reshape(-1)
    return waves, part


def dft_tables(lon_points, degrees, lat_count):
    waves, part = row_waves(degrees, lat_count)
    lon_ids = jnp.arange(lon_points)
    arg = (2.0 * math.pi / lon_points) * ((waves[:, None] * lon_ids[None, :]) % lon_points).astype(jnp.float32)
    value = jnp.where(part[:, None] == 0, jnp.cos(arg), -jnp.sin(arg))
    weight = jnp.where(waves == 0, 1.0, 2.0).astype(jnp.float32)
    return value.astype(jnp.bfloat16), (weight[:, None] * value).astype(jnp.bfloat16)


def entry_barrier(lon_count, lat_count):
    k, d = lax.axis_index('lon'), lax.axis_index('lat')
    sem = pltpu.get_barrier_semaphore()
    for q in range(1, lon_count):
        pl.semaphore_signal(sem, inc=1, device_id={'lon': lax.rem(k + q, lon_count)}, device_id_type=MESH)
    for e in range(1, lat_count):
        pl.semaphore_signal(sem, inc=1, device_id={'lat': lax.rem(d + e, lat_count)}, device_id_type=MESH)
    pl.semaphore_wait(sem, lon_count - 1 + lat_count - 1)


def lat_order(lat_count):
    order = [e for pair in zip(range(2, lat_count, 1), range(lat_count - 2, 0, -1)) for e in pair]
    order = list(dict.fromkeys(order))
    return order + [e for e in range(1, lat_count) if e not in order]


def lon_order(lon_count):
    order = []
    for q in range(1, lon_count // 2 + 1):
        order += [q, lon_count - q]
    return list(dict.fromkeys(order))


def to_spectral_kernel(lon_count, lat_count, t_loc, x_ref, dft_ref, out_ref, xin, xs, xr, stage, fb,
                       load_sem, y_send, y_recv, x_send, x_recv, keep_sem):
    k, d = lax.axis_index('lon'), lax.axis_index('lat')
    samples = x_ref.shape[0]
    channels = x_ref.shape[1] // t_loc
    halves, t_groups = channels // LANES, t_loc // ROWS
    rows = fb.shape[1]
    half_rows = LANES * t_loc

    loads = []
    for h in range(halves):
        for q in range(samples):
            src_s = lax.rem(k + q, lon_count)
            part = pl.ds(h * half_rows, half_rows)
            loads.append(pltpu.make_async_copy(x_ref.at[src_s, part], xin.at[q, part], load_sem.at[h, q]))
    for copy in loads:
        copy.start()
    entry_barrier(lon_count, lat_count)

    chunks = [(h, g) for h in range(halves) for g in range(t_groups)]
    y_copies = []
    for n, (h, g) in enumerate(chunks):
        sent = {}
        for q in lon_order(lon_count) + [0]:
            if g == 0:
                loads[h * samples + q].wait()

            def narrow(i, carry, q=q, h=h, g=g):
                t = g * ROWS + i
                block = xin[q, pl.ds(h * half_rows + t, LANES, stride=t_loc), :].astype(jnp.bfloat16)
                if q == 0:
                    xr[k, t, pl.ds(h * LANES, LANES), :] = block
                else:
                    xs[q - 1, t, pl.ds(h * LANES, LANES), :] = block
                return carry

            lax.fori_loop(0, ROWS, narrow, 0)
            if q:
                part = (pl.ds(g * ROWS, ROWS), pl.ds(h * LANES, LANES))
                sent[q] = pltpu.make_async_remote_copy(
                    src_ref=xs.at[(q - 1,) + part], dst_ref=xr.at[(k,) + part],
                    send_sem=y_send.at[n, q - 1], recv_sem=y_recv.at[n, q - 1],
                    device_id={'lon': lax.rem(k + q, lon_count)}, device_id_type=MESH)
                sent[q].start()
        y_copies.append(sent)

    kept, x_copies = [], []
    for n, (h, g) in enumerate(chunks):
        for q in range(1, lon_count):
            y_copies[n][q].wait_recv()

        def transform(i, carry, h=h, g=g):
            t = g * ROWS + i
            cols = jnp.concatenate([xr[b, t, pl.ds(h * LANES, LANES), :] for b in range(lon_count)], axis=1)
            spec = lax.dot_general(dft_ref[...], cols, (((1,), (1,)), ((), ())), preferred_element_type=jnp.float32)
            stage[pl.ds(i, lat_count * rows, stride=ROWS), :] = spec
            return carry

        lax.fori_loop(0, ROWS, transform, 0)
        for e in lat_order(lat_count) + [0]:
            dd = lax.rem(d + e, lat_count)

            def pack(r, carry, e=e, dd=dd, h=h, g=g):
                first = pl.multiple_of(dd * (rows * ROWS) + r * (8 * ROWS), ROWS)
                block = stage[pl.ds(first, 8 * ROWS), :].astype(jnp.bfloat16)
                fb[e, pl.ds(r * 8, 8), pl.ds(g * ROWS, ROWS), pl.ds(h * LANES, LANES)] = block.reshape(8, ROWS, LANES)
                return carry

            lax.fori_loop(0, rows // 8, pack, 0)
            src = fb.at[e, :, pl.ds(g * ROWS, ROWS), pl.ds(h * LANES, LANES)]
            dst = out_ref.at[:, pl.ds(pl.multiple_of(d * t_loc + g * ROWS, ROWS), ROWS), pl.ds(h * LANES, LANES)]
            if e == 0:
                copy = pltpu.make_async_copy(src, dst, keep_sem.at[n])
                kept.append(copy)
            else:
                copy = pltpu.make_async_remote_copy(
                    src_ref=src, dst_ref=dst, send_sem=x_send.at[n, e - 1], recv_sem=x_recv.at[n, e - 1],
                    device_id={'lat': dd}, device_id_type=MESH)
                x_copies.append(copy)
            copy.start()
    for sent in y_copies:
        for q in range(1, lon_count):
            sent[q].wait_send()
    for copy in kept:
        copy.wait()
    for copy in x_copies:
        copy.wait_send()
        copy.wait_recv()


def to_grid_kernel(lon_count, lat_count, t_loc, g_ref, dft_ref, out_ref, gr, stage, ys,
                   load_sem, x_send, x_recv, y_send, y_recv, keep_sem):
    k, d = lax.axis_index('lon'), lax.axis_index('lat')
    rows, channels = g_ref.shape[1], g_ref.shape[2]
    halves, t_groups = channels // LANES, t_loc // ROWS
    entry_barrier(lon_count, lat_count)
    chunks = [(h, g) for h in range(halves) for g in range(t_groups)]
    own, x_copies = [], []
    for n, (h, g) in enumerate(chunks):
        sent = []
        for e in lat_order(lat_count) + [0]:
            dd = lax.rem(d + e, lat_count)
            src = g_ref.at[pl.ds(dd * t_loc + g * ROWS, ROWS), :, pl.ds(h * LANES, LANES)]
            dst = gr.at[pl.ds(g * ROWS, ROWS), pl.ds(pl.multiple_of(d * rows, ROWS), rows), pl.ds(h * LANES, LANES)]
            if e == 0:
                copy = pltpu.make_async_copy(src, dst, load_sem.at[n])
                own.append(copy)
            else:
                copy = pltpu.make_async_remote_copy(
                    src_ref=src, dst_ref=dst, send_sem=x_send.at[n, e - 1], recv_sem=x_recv.at[n, e - 1],
                    device_id={'lat': dd}, device_id_type=MESH)
                sent.append(copy)
            copy.start()
        x_copies.append(sent)

    kept, y_copies = [], []
    for n, (h, g) in enumerate(chunks):
        own[n].wait()
        for copy in x_copies[n]:
            copy.wait_recv()

        def transform(i, carry, h=h, g=g):
            spec = gr[g * ROWS + i, :, pl.ds(h * LANES, LANES)]
            wave = lax.dot_general(spec, dft_ref[...], (((0,), (0,)), ((), ())), preferred_element_type=jnp.float32)
            for b in range(lon_count):
                stage[b, pl.ds(i, LANES, stride=ROWS), :] = wave[:, b * LANES:(b + 1) * LANES]
            return carry

        lax.fori_loop(0, ROWS, transform, 0)
        for q in lon_order(lon_count) + [0]:
            kk = lax.rem(k + q, lon_count)

            def pack(r, carry, q=q, kk=kk, h=h, g=g):
                block = stage[kk, pl.ds(pl.multiple_of(r * (8 * ROWS), ROWS), 8 * ROWS), :].astype(jnp.bfloat16)
                ys[q, pl.ds(h * LANES + r * 8, 8), pl.ds(g * ROWS, ROWS), :] = block.reshape(8, ROWS, LANES)
                return carry

            lax.fori_loop(0, LANES // 8, pack, 0)
            part = (pl.ds(h * LANES, LANES), pl.ds(g * ROWS, ROWS))
            src, dst = ys.at[(q,) + part], out_ref.at[(k,) + part]
            if q == 0:
                copy = pltpu.make_async_copy(src, dst, keep_sem.at[n])
                kept.append(copy)
            else:
                copy = pltpu.make_async_remote_copy(
                    src_ref=src, dst_ref=dst, send_sem=y_send.at[n, q - 1], recv_sem=y_recv.at[n, q - 1],
                    device_id={'lon': kk}, device_id_type=MESH)
                y_copies.append(copy)
            copy.start()
    for sent in x_copies:
        for copy in sent:
            copy.wait_send()
    for copy in kept:
        copy.wait()
    for copy in y_copies:
        copy.wait_send()
        copy.wait_recv()


def legendre_kernel(transposed, base_ref, table_ref, in_ref, out_ref, stage):
    i = pl.program_id(1)
    table = table_ref[0].astype(jnp.bfloat16)
    dims = (((0,), (0,)), ((), ())) if transposed else (((1,), (0,)), ((), ()))
    size = out_ref.shape[0]
    halves = in_ref.shape[4] // LANES
    for r in range(2):
        res = lax.dot_general(table, in_ref[0, r, 0], dims, preferred_element_type=jnp.float32)
        for h in range(halves):
            stage[r, h, pl.ds(i, size, stride=ROWS), :] = res[:, h * LANES:(h + 1) * LANES]

    @pl.when(i == ROWS - 1)
    def _():
        def pack(n, carry):
            for r in range(2):
                for h in range(halves):
                    block = stage[r, h, pl.ds(pl.multiple_of(n * (8 * ROWS), ROWS), 8 * ROWS), :].astype(jnp.bfloat16)
                    out_ref[pl.ds(n * 8, 8), pl.ds(r * ROWS, ROWS), pl.ds(h * LANES, LANES)] = block.reshape(8, ROWS, LANES)
            return carry

        lax.fori_loop(0, size // 8, pack, 0)


def legendre(table, values, base, transposed):
    groups, _, _, length, channels = values.shape
    size = table.shape[2] if transposed else table.shape[1]
    return pl.pallas_call(
        functools.partial(legendre_kernel, transposed),
        out_shape=jax.ShapeDtypeStruct((size, groups * 2 * ROWS, channels), jnp.bfloat16),
        grid_spec=pltpu.PrefetchScalarGridSpec(
            num_scalar_prefetch=1, grid=(groups, ROWS),
            in_specs=[
                pl.BlockSpec((1,) + table.shape[1:], lambda g, i, base_ref: (base_ref[0] + g * ROWS + i, 0, 0)),
                pl.BlockSpec((1, 2, 1, length, channels), lambda g, i, base_ref: (g, 0, i, 0, 0)),
            ],
            out_specs=pl.BlockSpec((size, 2 * ROWS, channels), lambda g, i, base_ref: (0, g, 0)),
            scratch_shapes=[pltpu.VMEM((2, channels // LANES, size * ROWS, LANES), jnp.float32)]),
        compiler_params=pltpu.CompilerParams(vmem_limit_bytes=VMEM_LIMIT),
        name='legendre_back' if transposed else 'legendre_fwd',
    )(base, table, values)


def mix_kernel(w_ref, a_ref, out_ref, stage):
    rows, channels = a_ref.shape[1], a_ref.shape[2]
    tiles = channels // LANES
    stride = 2 * tiles

    def degree(n, carry):
        def weight(r):
            pieces = [w_ref[pl.ds(n * channels * stride + 2 * b + r, channels, stride=stride), :] for b in range(tiles)]
            return jnp.concatenate([p.astype(jnp.bfloat16) for p in pieces], axis=1)

        val = a_ref[n]
        turned = []
        for first in range(0, rows, 2 * ROWS):
            turned += [-val[first + ROWS:first + 2 * ROWS], val[first:first + ROWS]]
        turned = jnp.concatenate(turned, axis=0)
        dims = (((1,), (1,)), ((), ()))
        res = lax.dot_general(val, weight(0), dims, preferred_element_type=jnp.float32)
        res = res + lax.dot_general(turned, weight(1), dims, preferred_element_type=jnp.float32)
        for h in range(tiles):
            stage[h, pl.ds(n, rows, stride=ROWS), :] = res[:, h * LANES:(h + 1) * LANES]
        return carry

    lax.fori_loop(0, ROWS, degree, 0)
    for h in range(tiles):
        out_ref[:, :, h * LANES:(h + 1) * LANES] = stage[h].astype(jnp.bfloat16).reshape(rows, ROWS, LANES)


def mix(w_rows, coef):
    degrees, rows, channels = coef.shape
    per_degree = w_rows.shape[0] // degrees
    return pl.pallas_call(
        mix_kernel,
        out_shape=jax.ShapeDtypeStruct((rows, degrees, channels), jnp.bfloat16),
        grid=(degrees // ROWS,),
        in_specs=[
            pl.BlockSpec((ROWS * per_degree, LANES), lambda n: (n, 0)),
            pl.BlockSpec((ROWS, rows, channels), lambda n: (n, 0, 0)),
        ],
        out_specs=pl.BlockSpec((rows, ROWS, channels), lambda n: (0, n, 0)),
        scratch_shapes=[pltpu.VMEM((channels // LANES, rows * ROWS, LANES), jnp.float32)],
        compiler_params=pltpu.CompilerParams(vmem_limit_bytes=VMEM_LIMIT),
        name='mix',
    )(w_rows, coef)


def solution(mesh):
    lon_count, lat_count = mesh.shape['lon'], mesh.shape['lat']
    grid_spec = P('member', None, 'lat', 'lon')
    any_spec = pl.BlockSpec(memory_space=pl.ANY)
    vmem_spec = pl.BlockSpec(memory_space=pltpu.VMEM)
    dma = pltpu.SemaphoreType.DMA

    def local_layer(field_in, fwd_table, inv_table, mix_weights):
        samples, channels, t_loc, j_loc = field_in.shape
        degrees, latitudes = fwd_table.shape[1], fwd_table.shape[2]
        lon_points = j_loc * lon_count
        m_loc = degrees // lat_count
        groups, rows = m_loc // ROWS, 2 * m_loc
        n_chunks = (channels // LANES) * (t_loc // ROWS)
        fwd_dft, inv_dft = dft_tables(lon_points, degrees, lat_count)
        base = (lax.axis_index('lat') * m_loc).astype(jnp.int32).reshape(1)

        spec = pl.pallas_call(
            functools.partial(to_spectral_kernel, lon_count, lat_count, t_loc),
            out_shape=jax.ShapeDtypeStruct((rows, latitudes, channels), jnp.bfloat16),
            in_specs=[any_spec, vmem_spec],
            out_specs=any_spec,
            scratch_shapes=[
                pltpu.VMEM((samples, channels * t_loc, j_loc), jnp.float32),
                pltpu.VMEM((samples - 1, t_loc, channels, j_loc), jnp.bfloat16),
                pltpu.VMEM((lon_count, t_loc, channels, j_loc), jnp.bfloat16),
                pltpu.VMEM((lat_count * rows * ROWS, LANES), jnp.float32),
                pltpu.VMEM((lat_count, rows, t_loc, channels), jnp.bfloat16),
                dma((channels // LANES, samples)),
                dma((n_chunks, lon_count - 1)), dma((n_chunks, lon_count - 1)),
                dma((n_chunks, lat_count - 1)), dma((n_chunks, lat_count - 1)),
                dma((n_chunks,)),
            ],
            compiler_params=pltpu.CompilerParams(collective_id=0, has_side_effects=True, vmem_limit_bytes=VMEM_LIMIT),
            name='to_spectral',
        )(field_in.reshape(samples, channels * t_loc, j_loc), fwd_dft)

        coef = legendre(fwd_table, spec.reshape(groups, 2, ROWS, latitudes, channels), base, False)
        w_rows = mix_weights.reshape(degrees, channels, channels // LANES, LANES, 2)
        w_rows = jnp.transpose(w_rows, (0, 1, 2, 4, 3)).reshape(-1, LANES)
        mixed = mix(w_rows, coef)
        back = legendre(inv_table, mixed.reshape(groups, 2, ROWS, degrees, channels), base, True)

        wave = pl.pallas_call(
            functools.partial(to_grid_kernel, lon_count, lat_count, t_loc),
            out_shape=jax.ShapeDtypeStruct((samples, channels, t_loc, j_loc), jnp.bfloat16),
            in_specs=[any_spec, vmem_spec],
            out_specs=any_spec,
            scratch_shapes=[
                pltpu.VMEM((t_loc, lat_count * rows, channels), jnp.bfloat16),
                pltpu.VMEM((lon_count, LANES * ROWS, LANES), jnp.float32),
                pltpu.VMEM((lon_count, channels, t_loc, j_loc), jnp.bfloat16),
                dma((n_chunks,)),
                dma((n_chunks, lat_count - 1)), dma((n_chunks, lat_count - 1)),
                dma((n_chunks, lon_count - 1)), dma((n_chunks, lon_count - 1)),
                dma((n_chunks,)),
            ],
            compiler_params=pltpu.CompilerParams(collective_id=1, has_side_effects=True, vmem_limit_bytes=VMEM_LIMIT),
            name='to_grid',
        )(back, inv_dft)
        return field_in + jax.nn.gelu(wave.astype(jnp.float32), approximate=True)

    whole = P(None, None, None)
    return jax.shard_map(local_layer, mesh=mesh, in_specs=(grid_spec, whole, whole, P(None, None, None, None)),
                         out_specs=grid_spec, check_vma=False)
```

```python
import functools
import math
import jax
import jax.numpy as jnp
from jax import lax
from jax.experimental import pallas as pl
from jax.experimental.pallas import tpu as pltpu
from jax.sharding import PartitionSpec as P

MESH = pl.DeviceIdType.MESH
ROWS = 16
T_ROWS = 8
PITCH = 17
WAVES = 4
LANES = 128
VMEM_LIMIT = 66000000


def row_waves(degrees, lat_count):
    m_loc = degrees // lat_count
    groups = m_loc // ROWS
    waves = jnp.arange(degrees).reshape(lat_count, groups, 1, ROWS)
    waves = jnp.broadcast_to(waves, (lat_count, groups, 2, ROWS)).reshape(-1)
    part = jnp.broadcast_to(jnp.arange(2).reshape(1, 1, 2, 1), (lat_count, groups, 2, ROWS)).reshape(-1)
    return waves, part


def dft_tables(lon_points, degrees, lat_count):
    waves, part = row_waves(degrees, lat_count)
    lon_ids = jnp.arange(lon_points)
    arg = (2.0 * math.pi / lon_points) * ((waves[:, None] * lon_ids[None, :]) % lon_points).astype(jnp.float32)
    value = jnp.where(part[:, None] == 0, jnp.cos(arg), -jnp.sin(arg))
    weight = jnp.where(waves == 0, 1.0, 2.0).astype(jnp.float32)
    return value.astype(jnp.bfloat16), (weight[:, None] * value).astype(jnp.bfloat16)


def entry_barrier(lon_count, lat_count):
    k, d = lax.axis_index('lon'), lax.axis_index('lat')
    sem = pltpu.get_barrier_semaphore()
    for q in range(1, lon_count):
        pl.semaphore_signal(sem, inc=1, device_id={'lon': lax.rem(k + q, lon_count)}, device_id_type=MESH)
    for e in range(1, lat_count):
        pl.semaphore_signal(sem, inc=1, device_id={'lat': lax.rem(d + e, lat_count)}, device_id_type=MESH)
    pl.semaphore_wait(sem, lon_count - 1 + lat_count - 1)


def lat_order(lat_count):
    order = [e for pair in zip(range(2, lat_count, 1), range(lat_count - 2, 0, -1)) for e in pair]
    order = list(dict.fromkeys(order))
    return order + [e for e in range(1, lat_count) if e not in order]


def lon_order(lon_count):
    order = []
    for q in range(1, lon_count // 2 + 1):
        order += [q, lon_count - q]
    return list(dict.fromkeys(order))


def to_spectral_kernel(lon_count, lat_count, t_loc, x_ref, dft_ref, out_ref, xin, xs, xr, stage, fb,
                       load_sem, y_send, y_recv, x_send, x_recv, keep_sem):
    k, d = lax.axis_index('lon'), lax.axis_index('lat')
    samples = x_ref.shape[0]
    channels = x_ref.shape[1] // t_loc
    halves, t_groups = channels // LANES, t_loc // T_ROWS
    rows = fb.shape[1]
    half_rows = LANES * t_loc

    loads = []
    for h in range(halves):
        for q in range(samples):
            src_s = lax.rem(k + q, lon_count)
            part = pl.ds(h * half_rows, half_rows)
            loads.append(pltpu.make_async_copy(x_ref.at[src_s, part], xin.at[q, part], load_sem.at[h, q]))
    for copy in loads:
        copy.start()
    entry_barrier(lon_count, lat_count)

    chunks = [(h, g) for h in range(halves) for g in range(t_groups)]
    y_copies = []
    for n, (h, g) in enumerate(chunks):
        sent = {}
        for q in lon_order(lon_count) + [0]:
            if g == 0:
                loads[h * samples + q].wait()

            def narrow(i, carry, q=q, h=h, g=g):
                t = g * T_ROWS + i
                block = xin[q, pl.ds(h * half_rows + t, LANES, stride=t_loc), :].astype(jnp.bfloat16)
                if q == 0:
                    xr[k, t, pl.ds(h * LANES, LANES), :] = block
                else:
                    xs[q - 1, t, pl.ds(h * LANES, LANES), :] = block
                return carry

            lax.fori_loop(0, T_ROWS, narrow, 0)
            if q:
                part = (pl.ds(g * T_ROWS, T_ROWS), pl.ds(h * LANES, LANES))
                sent[q] = pltpu.make_async_remote_copy(
                    src_ref=xs.at[(q - 1,) + part], dst_ref=xr.at[(k,) + part],
                    send_sem=y_send.at[n, q - 1], recv_sem=y_recv.at[n, q - 1],
                    device_id={'lon': lax.rem(k + q, lon_count)}, device_id_type=MESH)
                sent[q].start()
        y_copies.append(sent)

    kept, x_copies = [], []
    for n, (h, g) in enumerate(chunks):
        for q in range(1, lon_count):
            y_copies[n][q].wait_recv()

        def transform(i, carry, h=h, g=g):
            t = g * T_ROWS + i
            cols = jnp.concatenate([xr[b, t, pl.ds(h * LANES, LANES), :] for b in range(lon_count)], axis=1)
            spec = lax.dot_general(dft_ref[...], cols, (((1,), (1,)), ((), ())), preferred_element_type=jnp.float32)
            stage[pl.ds(i, lat_count * rows, stride=T_ROWS), :] = spec
            return carry

        lax.fori_loop(0, T_ROWS, transform, 0)
        for e in lat_order(lat_count) + [0]:
            dd = lax.rem(d + e, lat_count)

            def pack(r, carry, e=e, dd=dd, h=h, g=g):
                first = pl.multiple_of(dd * (rows * T_ROWS) + r * (8 * T_ROWS), T_ROWS)
                block = stage[pl.ds(first, 8 * T_ROWS), :].reshape(8, T_ROWS, LANES)
                fb[e, pl.ds(r * 8, 8), pl.ds(g * T_ROWS, T_ROWS), pl.ds(h * LANES, LANES)] = block.astype(jnp.bfloat16)
                return carry

            lax.fori_loop(0, rows // 8, pack, 0)
            src = fb.at[e, :, pl.ds(g * T_ROWS, T_ROWS), pl.ds(h * LANES, LANES)]
            dst = out_ref.at[:, pl.ds(pl.multiple_of(d * t_loc + g * T_ROWS, T_ROWS), T_ROWS), pl.ds(h * LANES, LANES)]
            if e == 0:
                copy = pltpu.make_async_copy(src, dst, keep_sem.at[n])
                kept.append(copy)
            else:
                copy = pltpu.make_async_remote_copy(
                    src_ref=src, dst_ref=dst, send_sem=x_send.at[n, e - 1], recv_sem=x_recv.at[n, e - 1],
                    device_id={'lat': dd}, device_id_type=MESH)
                x_copies.append(copy)
            copy.start()
    for sent in y_copies:
        for q in range(1, lon_count):
            sent[q].wait_send()
    for copy in kept:
        copy.wait()
    for copy in x_copies:
        copy.wait_send()
        copy.wait_recv()


def mix_to_grid_kernel(lon_count, lat_count, t_loc, coef_ref, w_ref, table_ref, dft_ref, out_ref,
                       wbuf, abuf, mixed, mstage, tables, lstage, gs, gr, ystage, ys,
                       w_sem, a_sem, table_sem, x_send, x_recv, y_send, y_recv, keep_sem):
    k, d = lax.axis_index('lon'), lax.axis_index('lat')
    degrees, rows, channels = coef_ref.shape
    latitudes, m_loc = table_ref.shape[2], tables.shape[0]
    halves, t_groups, tiles = channels // LANES, t_loc // T_ROWS, channels // LANES
    groups, blocks = m_loc // ROWS, degrees // ROWS
    per_half = LANES * 2 * tiles
    nt = (((1,), (1,)), ((), ()))
    tn = (((0,), (0,)), ((), ()))

    def fetch(n):
        h, b, slot = lax.div(n, blocks), lax.rem(n, blocks), lax.rem(n, 2)
        degs = pl.ds(pl.multiple_of(b * ROWS, ROWS), ROWS)
        part = pl.ds(pl.multiple_of(h * per_half, per_half), per_half)
        return (pltpu.make_async_copy(w_ref.at[degs, part], wbuf.at[slot], w_sem.at[slot]),
                pltpu.make_async_copy(coef_ref.at[degs], abuf.at[slot], a_sem.at[slot]))

    for copy in fetch(0):
        copy.start()
    load_tables = pltpu.make_async_copy(table_ref.at[pl.ds(d * m_loc, m_loc)], tables, table_sem)
    load_tables.start()
    entry_barrier(lon_count, lat_count)

    def mix(h, first, last):
        def block(b, carry):
            n = h * blocks + b
            slot = lax.rem(n, 2)

            @pl.when(n + 1 < halves * blocks)
            def _():
                for copy in fetch(n + 1):
                    copy.start()

            for copy in fetch(n):
                copy.wait()

            def degree(u, carry):
                w = jnp.concatenate([
                    jnp.concatenate([
                        wbuf[slot, u, pl.ds(2 * i + r, LANES, stride=2 * tiles), :].astype(jnp.bfloat16)
                        for i in range(tiles)], axis=1)
                    for r in range(2)], axis=0)
                res = lax.dot_general(abuf[slot, u], w, nt, preferred_element_type=jnp.float32)
                parts = []
                for f in range(0, rows, 2 * ROWS):
                    re, im = res[f:f + ROWS], res[f + ROWS:f + 2 * ROWS]
                    parts += [re[:, :LANES] - im[:, LANES:], im[:, :LANES] + re[:, LANES:]]
                mstage[pl.ds(u, rows, stride=PITCH), :] = jnp.concatenate(parts, axis=0)
                return carry

            lax.fori_loop(0, ROWS, degree, 0, unroll=8)
            degs = pl.ds(pl.multiple_of(b * ROWS, ROWS), ROWS)
            for row in range(rows):
                mixed[row, degs, :] = mstage[row * PITCH:row * PITCH + ROWS, :].astype(jnp.bfloat16)
            return carry

        lax.fori_loop(first, last, block, 0)

    def legendre_back(h):
        lanes = pl.ds(h * LANES, LANES)
        for gi in range(groups):
            def wave(w, carry):
                table = tables[gi * ROWS + w].astype(jnp.bfloat16)
                both = jnp.concatenate([mixed[gi * 2 * ROWS + w], mixed[gi * 2 * ROWS + ROWS + w]], axis=1)
                res = lax.dot_general(table, both, tn, preferred_element_type=jnp.float32)
                for r in range(2):
                    lstage[r, pl.ds(w, latitudes, stride=PITCH), :] = res[:, r * LANES:(r + 1) * LANES]
                return carry

            lax.fori_loop(0, ROWS, wave, 0, unroll=4)

            def pack(n, carry):
                for u in range(8):
                    for r in range(2):
                        block = lstage[r, pl.ds((n * 8 + u) * PITCH, ROWS), :].astype(jnp.bfloat16)
                        gs[n * 8 + u, pl.ds((gi * 2 + r) * ROWS, ROWS), lanes] = block
                return carry

            lax.fori_loop(0, latitudes // 8, pack, 0)

        def own(t, carry):
            gr[t, pl.ds(pl.multiple_of(d * rows, ROWS), rows), lanes] = gs[d * t_loc + t, :, lanes]
            return carry

        lax.fori_loop(0, t_loc, own, 0)

    x_copies, y_copies, kept = {}, [], []

    def send_lat(h):
        for g in range(t_groups):
            n, lanes = h * t_groups + g, pl.ds(h * LANES, LANES)
            sent = []
            for e in lat_order(lat_count):
                dd = lax.rem(d + e, lat_count)
                sent.append(pltpu.make_async_remote_copy(
                    src_ref=gs.at[pl.ds(dd * t_loc + g * T_ROWS, T_ROWS), :, lanes],
                    dst_ref=gr.at[pl.ds(g * T_ROWS, T_ROWS), pl.ds(pl.multiple_of(d * rows, ROWS), rows), lanes],
                    send_sem=x_send.at[n, e - 1], recv_sem=x_recv.at[n, e - 1],
                    device_id={'lat': dd}, device_id_type=MESH))
                sent[-1].start()
            x_copies[n] = sent

    def to_grid(h, g):
        n = h * t_groups + g
        for copy in x_copies[n]:
            copy.wait_recv()

        def transform(i, carry):
            spec = gr[g * T_ROWS + i, :, pl.ds(h * LANES, LANES)]
            wave = lax.dot_general(spec, dft_ref[...], tn, preferred_element_type=jnp.float32)
            for b in range(lon_count):
                ystage[b, pl.ds(i, LANES, stride=T_ROWS), :] = wave[:, b * LANES:(b + 1) * LANES]
            return carry

        lax.fori_loop(0, T_ROWS, transform, 0)
        for q in lon_order(lon_count) + [0]:
            kk = lax.rem(k + q, lon_count)

            def pack(r, carry, q=q, kk=kk):
                block = ystage[kk, pl.ds(pl.multiple_of(r * (8 * T_ROWS), T_ROWS), 8 * T_ROWS), :]
                block = block.reshape(8, T_ROWS, LANES).astype(jnp.bfloat16)
                ys[q, pl.ds(h * LANES + r * 8, 8), pl.ds(g * T_ROWS, T_ROWS), :] = block
                return carry

            lax.fori_loop(0, LANES // 8, pack, 0)
            part = (pl.ds(h * LANES, LANES), pl.ds(g * T_ROWS, T_ROWS))
            src, dst = ys.at[(q,) + part], out_ref.at[(k,) + part]
            if q == 0:
                copy = pltpu.make_async_copy(src, dst, keep_sem.at[n])
                kept.append(copy)
            else:
                copy = pltpu.make_async_remote_copy(
                    src_ref=src, dst_ref=dst, send_sem=y_send.at[n, q - 1], recv_sem=y_recv.at[n, q - 1],
                    device_id={'lon': kk}, device_id_type=MESH)
                y_copies.append(copy)
            copy.start()

    pending = []
    for h in range(halves):
        if h == 0:
            mix(h, 0, blocks)
            load_tables.wait()
        else:
            cuts = [0, blocks // 2, 3 * blocks // 4, blocks]
            for first, last in zip(cuts, cuts[1:]):
                mix(h, first, last)
                if pending:
                    to_grid(*pending.pop(0))
        legendre_back(h)
        send_lat(h)
        pending += [(h, g) for g in range(t_groups)]
    for chunk in pending:
        to_grid(*chunk)
    for sent in x_copies.values():
        for copy in sent:
            copy.wait_send()
    for copy in kept:
        copy.wait()
    for copy in y_copies:
        copy.wait_send()
        copy.wait_recv()


def legendre_kernel(transposed, base_ref, table_ref, in_ref, out_ref, stage):
    step = pl.program_id(1)
    dims = (((0,), (0,)), ((), ())) if transposed else (((1,), (0,)), ((), ()))
    size = out_ref.shape[0]
    halves = in_ref.shape[4] // LANES
    for w in range(WAVES):
        table = table_ref[w].astype(jnp.bfloat16)
        for r in range(2):
            res = lax.dot_general(table, in_ref[0, r, w], dims, preferred_element_type=jnp.float32)
            for h in range(halves):
                stage[r, h, pl.ds(step * WAVES + w, size, stride=PITCH), :] = res[:, h * LANES:(h + 1) * LANES]

    @pl.when(step == ROWS // WAVES - 1)
    def _():
        def pack(n, carry):
            for r in range(2):
                for h in range(halves):
                    for u in range(8):
                        block = stage[r, h, pl.ds((n * 8 + u) * PITCH, ROWS), :].astype(jnp.bfloat16)
                        out_ref[n * 8 + u, pl.ds(r * ROWS, ROWS), pl.ds(h * LANES, LANES)] = block
            return carry

        lax.fori_loop(0, size // 8, pack, 0)


def legendre(table, values, base, transposed):
    groups, _, _, length, channels = values.shape
    size = table.shape[2] if transposed else table.shape[1]
    return pl.pallas_call(
        functools.partial(legendre_kernel, transposed),
        out_shape=jax.ShapeDtypeStruct((size, groups * 2 * ROWS, channels), jnp.bfloat16),
        grid_spec=pltpu.PrefetchScalarGridSpec(
            num_scalar_prefetch=1, grid=(groups, ROWS // WAVES),
            in_specs=[
                pl.BlockSpec((WAVES,) + table.shape[1:], lambda g, i, base_ref: (base_ref[0] + g * (ROWS // WAVES) + i, 0, 0)),
                pl.BlockSpec((1, 2, WAVES, length, channels), lambda g, i, base_ref: (g, 0, i, 0, 0)),
            ],
            out_specs=pl.BlockSpec((size, 2 * ROWS, channels), lambda g, i, base_ref: (0, g, 0)),
            scratch_shapes=[pltpu.VMEM((2, channels // LANES, size * PITCH, LANES), jnp.float32)]),
        compiler_params=pltpu.CompilerParams(vmem_limit_bytes=VMEM_LIMIT),
        name='legendre_back' if transposed else 'legendre_fwd',
    )(base, table, values)


def solution(mesh):
    lon_count, lat_count = mesh.shape['lon'], mesh.shape['lat']
    grid_spec = P('member', None, 'lat', 'lon')
    any_spec = pl.BlockSpec(memory_space=pl.ANY)
    vmem_spec = pl.BlockSpec(memory_space=pltpu.VMEM)
    dma = pltpu.SemaphoreType.DMA

    def local_layer(field_in, fwd_table, inv_table, mix_weights):
        samples, channels, t_loc, j_loc = field_in.shape
        degrees, latitudes = fwd_table.shape[1], fwd_table.shape[2]
        lon_points = j_loc * lon_count
        m_loc = degrees // lat_count
        groups, rows = m_loc // ROWS, 2 * m_loc
        n_chunks = (channels // LANES) * (t_loc // T_ROWS)
        fwd_dft, inv_dft = dft_tables(lon_points, degrees, lat_count)
        base = (lax.axis_index('lat') * (m_loc // WAVES)).astype(jnp.int32).reshape(1)

        spec = pl.pallas_call(
            functools.partial(to_spectral_kernel, lon_count, lat_count, t_loc),
            out_shape=jax.ShapeDtypeStruct((rows, latitudes, channels), jnp.bfloat16),
            in_specs=[any_spec, vmem_spec],
            out_specs=any_spec,
            scratch_shapes=[
                pltpu.VMEM((samples, channels * t_loc, j_loc), jnp.float32),
                pltpu.VMEM((samples - 1, t_loc, channels, j_loc), jnp.bfloat16),
                pltpu.VMEM((lon_count, t_loc, channels, j_loc), jnp.bfloat16),
                pltpu.VMEM((lat_count * rows * T_ROWS, LANES), jnp.float32),
                pltpu.VMEM((lat_count, rows, t_loc, channels), jnp.bfloat16),
                dma((channels // LANES, samples)),
                dma((n_chunks, lon_count - 1)), dma((n_chunks, lon_count - 1)),
                dma((n_chunks, lat_count - 1)), dma((n_chunks, lat_count - 1)),
                dma((n_chunks,)),
            ],
            compiler_params=pltpu.CompilerParams(collective_id=0, has_side_effects=True, vmem_limit_bytes=VMEM_LIMIT),
            name='to_spectral',
        )(field_in.reshape(samples, channels * t_loc, j_loc), fwd_dft)

        coef = legendre(fwd_table, spec.reshape(groups, 2, ROWS, latitudes, channels), base, False)
        tiles = channels // LANES
        w_rows = mix_weights.reshape(degrees, channels, tiles, LANES, 2)
        w_rows = jnp.transpose(w_rows, (0, 1, 2, 4, 3)).reshape(degrees, channels * 2 * tiles, LANES)
        wave = pl.pallas_call(
            functools.partial(mix_to_grid_kernel, lon_count, lat_count, t_loc),
            out_shape=jax.ShapeDtypeStruct((samples, channels, t_loc, j_loc), jnp.bfloat16),
            in_specs=[any_spec, any_spec, any_spec, vmem_spec],
            out_specs=any_spec,
            scratch_shapes=[
                pltpu.VMEM((2, ROWS, LANES * 2 * tiles, LANES), jnp.float32),
                pltpu.VMEM((2, ROWS, rows, channels), jnp.bfloat16),
                pltpu.VMEM((rows, degrees, LANES), jnp.bfloat16),
                pltpu.VMEM((rows * PITCH, LANES), jnp.float32),
                pltpu.VMEM((m_loc, degrees, latitudes), jnp.float32),
                pltpu.VMEM((2, latitudes * PITCH, LANES), jnp.float32),
                pltpu.VMEM((latitudes, rows, channels), jnp.bfloat16),
                pltpu.VMEM((t_loc, lat_count * rows, channels), jnp.bfloat16),
                pltpu.VMEM((lon_count, LANES * T_ROWS, LANES), jnp.float32),
                pltpu.VMEM((lon_count, channels, t_loc, j_loc), jnp.bfloat16),
                dma((2,)), dma((2,)), dma,
                dma((n_chunks, lat_count - 1)), dma((n_chunks, lat_count - 1)),
                dma((n_chunks, lon_count - 1)), dma((n_chunks, lon_count - 1)),
                dma((n_chunks,)),
            ],
            compiler_params=pltpu.CompilerParams(collective_id=1, has_side_effects=True, vmem_limit_bytes=VMEM_LIMIT),
            name='mix_to_grid',
        )(coef, w_rows, inv_table, inv_dft)
        return field_in + jax.nn.gelu(wave.astype(jnp.float32), approximate=True)

    whole = P(None, None, None)
    return jax.shard_map(local_layer, mesh=mesh, in_specs=(grid_spec, whole, whole, P(None, None, None, None)),
                         out_specs=grid_spec, check_vma=False)
```
